128 devices in a mesh: seq: 8 (over x, z_lo), blk: 8 (over y, core), uly: 2 (over z_hi).
Axes of the slice: x: 4, y: 4, z: 4 (z_hi: 2, z_lo: 2; z = z_hi * 2 + z_lo), core: 2. Of those that a mesh axis runs over, the one named last changes fastest.
Arguments:
- queries: bfloat16 [32768, 5120], P(('seq', 'blk', 'uly')), parts along dimension 0, may hold values from -60 to 60, as said below
- keys: bfloat16 [32768, 1024], P(('seq', 'blk', 'uly')), parts along dimension 0, may hold values from -60 to 60, as said below
- values: bfloat16 [32768, 1024], P(('seq', 'blk', 'uly')), parts along dimension 0, may hold values from -6 to 6
- positions: int32 [3, 32768], P(None, ('seq', 'blk', 'uly')), parts along dimension 1, may hold values from 0 to 1038
- doc_lengths: int32 [64], P('seq'), parts along dimension 0, may hold values from 1 to 2048, 4096 in all
Outputs:
- attended: bfloat16 [32768, 5120], P(('seq', 'blk', 'uly')), parts along dimension 0
The draws below stay inside these ranges and needn't reach their ends.
There are 8 independent parts, one for each index of `seq`. The reference program is written for one: setup_inputs(seed, part) draws one part's arguments, and reference() takes and returns one part's arrays. A program takes and returns all parts, laid end to end along the dimension named above; each array names one. Nothing has to cross between parts.
Inputs may be any that keep to these rules, and one draw needn't show every extreme that they name: queries; the query rows hold values of order one, a few rows may be much larger. keys; the key rows hold values of order one, a few rows may be much larger.
All inputs are finite; a program needn't handle non-finite values.
Results may differ from the reference program's by a relative error of at most 0.0055.
Values may be sent and summed in bfloat16 or wider, within the bound.
A program may use at most 384 MiB of HBM per device.

```python
import math
import jax
import jax.numpy as jnp
import numpy as np
from jax import lax

KEY_VALUE_HEADS = 8
HEAD_SIZE = 128
QUERY_PER_KEY = 5
HQ = 40
NDOC = 8
PACKED_TOKENS = 4096


def draw_queries(key, part):
    frequency_base = jnp.clip(jax.random.normal(jax.random.fold_in(key, 1), (PACKED_TOKENS, HQ * HEAD_SIZE), jnp.float32), -6.0, 6.0)
    return frequency_base.astype(jnp.bfloat16)


def draw_keys(key, part):
    frequency_base = jnp.clip(jax.random.normal(jax.random.fold_in(key, 2), (PACKED_TOKENS, KEY_VALUE_HEADS * HEAD_SIZE), jnp.float32), -6.0, 6.0)
    return frequency_base.astype(jnp.bfloat16)


def draw_positions(key, part):
    index = jnp.arange(PACKED_TOKENS, dtype=jnp.int32)
    jitter = jax.random.randint(key, (3, PACKED_TOKENS), 0, 16)
    return (index[None, :] // 4 + jitter).astype(jnp.int32)


def shard_levels(own_key, shape, pieces, least, high):
    def one(axis_at, blocks):
        steps = jax.random.uniform(jax.random.fold_in(jax.random.fold_in(own_key, 6), axis_at), (blocks,), jnp.float32, least / len(pieces), high / len(pieces))
        return jnp.repeat(jnp.exp(steps), shape[axis_at] // blocks).reshape((-1,) + (1,) * (len(shape) - axis_at - 1))

    level = one(*pieces[0])
    for cut in pieces[1:]:
        level = level * one(*cut)
    return level


def profile(count, total, limit, lean):
    loads = [(1 << 20) // math.isqrt(standing ** lean) + 1 for standing in range(2, count + 1)]
    surplus, holding = total - limit - (count - 1), [1] * (count - 1)
    while surplus > 0:
        candidates = [i for i in range(count - 1) if holding[i] < limit]
        mass, remaining = sum([loads[i] for i in candidates]), surplus
        for i in candidates:
            more = min(limit - holding[i], max(1, remaining * loads[i] // mass), surplus)
            holding[i] = holding[i] + more
            surplus = surplus - more
    return np.array([limit] + holding)


def ragged(key, count, total, most, slope):
    if count == 2:
        one = jax.random.randint(key, (), max(1, total - most), min(most, total - 1) + 1)
        return jnp.stack([one, total - one])
    sizes = jnp.asarray(profile(count, total, most, slope), jnp.int32)
    pairs = (count - 1) // 2
    donor, sink = sizes[1:1 + 2 * pairs:2], sizes[2:2 + 2 * pairs:2]
    margin = jnp.minimum(donor - 1, most - sink)
    passed = jax.random.randint(jax.random.fold_in(key, 1), (pairs,), 0, 1 << 20) % (margin + 1)
    sizes = sizes.at[1:1 + 2 * pairs:2].set(donor - passed).at[2:2 + 2 * pairs:2].set(sink + passed)
    return sizes[jax.random.permutation(jax.random.fold_in(key, 2), count)]


def normal_values(own_key, shape, width, bound, shards=(), held_as=jnp.bfloat16):
    factor_of = shard_levels(own_key, shape, shards, -0.22, 0.18) if shards else 1.0
    values = jax.random.normal(own_key, shape, jnp.float32) * width * factor_of
    return jnp.minimum(jnp.maximum(values, -bound), bound).astype(held_as)


def setup_inputs(seed: int = 0, part: int = 0) -> dict:
    key_list = jax.random.split(jax.random.key(seed), 6)
    own_keys = jax.random.split(jax.random.fold_in(key_list[5], part), 6)
    return {
        "queries": draw_queries(jax.random.fold_in(jax.random.fold_in(key_list[5], part), 71), part),
        "keys": draw_keys(jax.random.fold_in(jax.random.fold_in(key_list[5], part), 71), part),
        "values": normal_values(own_keys[2], (PACKED_TOKENS, KEY_VALUE_HEADS * HEAD_SIZE), 1.0, 6.0, ((0, 16),)),
        "positions": draw_positions(jax.random.fold_in(jax.random.fold_in(key_list[5], part), 71), part),
        "doc_lengths": ragged(own_keys[4], NDOC, PACKED_TOKENS, PACKED_TOKENS // 2, 2).astype(jnp.int32),
    }


def apply_rotary(x, pos, heads):
    rows = x.shape[0]
    half = HEAD_SIZE // 2
    pair = jnp.arange(half, dtype=jnp.int32)
    freq = jnp.power(jnp.float32(1000000.0), -2.0 * pair.astype(jnp.float32) / HEAD_SIZE)
    place = pos.astype(jnp.float32)
    first = HEAD_SIZE // 8
    second = first + 3 * HEAD_SIZE // 16
    chosen = jnp.where(pair[None, :] < first, place[0][:, None], jnp.where(pair[None, :] < second, place[1][:, None], place[2][:, None]))
    angle = chosen * freq[None, :]
    cosine = jnp.cos(angle)[:, None, :]
    sine = jnp.sin(angle)[:, None, :]
    parts = x.reshape(rows, heads, HEAD_SIZE).astype(jnp.float32)
    lower = parts[..., :half]
    upper = parts[..., half:]
    turned = jnp.concatenate([lower * cosine - upper * sine, upper * cosine + lower * sine], axis=-1)
    return turned.reshape(rows, heads * HEAD_SIZE).astype(jnp.bfloat16)

def doc_starts(index, doc_lengths):
    ends = jnp.cumsum(doc_lengths).astype(jnp.int32)
    return lax.optimization_barrier(jnp.sum(jnp.where(ends[None, :] <= index[:, None], doc_lengths[None, :], 0), axis=1)).astype(jnp.int32)

def reference(queries, keys, values, positions, doc_lengths):
    query_rotated = apply_rotary(queries, positions, HQ)
    key_rotated = apply_rotary(keys, positions, KEY_VALUE_HEADS)
    index = jnp.arange(PACKED_TOKENS, dtype=jnp.int32)
    starts = doc_starts(index, doc_lengths)
    allowed = (index[None, :] <= index[:, None]) & (index[None, :] >= starts[:, None])
    scale = 1.0 / math.sqrt(HEAD_SIZE)
    grouped_query = jnp.transpose(query_rotated.reshape(PACKED_TOKENS, KEY_VALUE_HEADS, QUERY_PER_KEY, HEAD_SIZE), (1, 0, 2, 3))
    key_heads_view = jnp.transpose(key_rotated.reshape(PACKED_TOKENS, KEY_VALUE_HEADS, HEAD_SIZE), (1, 0, 2))
    value_heads_view = jnp.transpose(values.reshape(PACKED_TOKENS, KEY_VALUE_HEADS, HEAD_SIZE), (1, 0, 2))

    def one_head(operands):
        q_head, k_head, v_head = operands
        scores = jnp.einsum('rgd,bd->grb', q_head.astype(jnp.float32), k_head.astype(jnp.float32)) * scale
        scores = jnp.where(allowed[None], scores, -1e+30)
        best = lax.optimization_barrier(jnp.max(scores, axis=-1, keepdims=True))
        weights = jnp.where(allowed[None], jnp.exp(scores - best), 0.0)
        total = lax.optimization_barrier(jnp.sum(weights, axis=-1))
        weight_b = weights.astype(jnp.bfloat16)
        summed = jnp.einsum('grb,bd->grd', weight_b.astype(jnp.float32), v_head.astype(jnp.float32))
        return summed / total[..., None]
    result = lax.map(one_head, (grouped_query, key_heads_view, value_heads_view))
    return jnp.transpose(result, (2, 0, 1, 3)).reshape(PACKED_TOKENS, HQ * HEAD_SIZE).astype(jnp.bfloat16)
```

```python
import math

import jax
import jax.numpy as jnp
import numpy as np
from jax import lax
from jax.experimental import pallas as pl
from jax.experimental.pallas import tpu as pltpu
from jax.sharding import PartitionSpec as P

D = 128
G = 5
KH = 8
ROWS = 256
LAG = 2
HALF = D // 2
BIG = 3.0e38
LOW = -1.0e30
EXP_SCALE = math.log2(math.e) / math.sqrt(D)
MESH = pl.DeviceIdType.MESH
CONTRACT_LAST = (((1,), (1,)), ((), ()))
CONTRACT_FIRST = (((0,), (0,)), ((), ()))


def kernel(
    q_hbm, k_hbm, v_hbm, pos_ref, freq_ref, docs_ref, out_hbm,
    buf, qraw, qs, kraw, acc, best, total, masks, cos_t, sin_t, ostage,
    in_sem, v_sem, out_sem, send_sem, recv_sem,
):
    s = lax.axis_index("seq")
    blk = lax.axis_index("blk")
    z = lax.axis_index("uly")
    y = lax.div(blk, 2)
    c = lax.rem(blk, 2)
    own = 4 * y + 2 * c + z
    up = (s, 2 * lax.rem(y + 1, 4) + c, z)
    down = (s, 2 * lax.rem(y + 3, 4) + c, z)
    across = (s, blk, 1 - z)
    sibling = (s, 2 * y + 1 - c, z)
    links = (up, down, across, sibling)

    def slot(back, core, zz):
        return 4 * lax.rem(y + 4 - back, 4) + 2 * zz + core

    own_slot = slot(0, c, z)

    k_copy = pltpu.make_async_copy(k_hbm, kraw, in_sem.at[0])
    k_copy.start()
    v_copies = [
        pltpu.make_async_copy(
            v_hbm.at[:, h * D:(h + 1) * D], buf.at[own_slot, h, ROWS:2 * ROWS, :], v_sem.at[h]
        )
        for h in range(KH)
    ]
    for copy in v_copies:
        copy.start()
    q_copy = pltpu.make_async_copy(q_hbm, qraw, in_sem.at[1])
    q_copy.start()

    barrier = pltpu.get_barrier_semaphore()
    for peer in links:
        pl.semaphore_signal(barrier, inc=1, device_id=peer, device_id_type=MESH)

    pair = lax.broadcasted_iota(jnp.int32, (HALF, ROWS), 0)
    place = pos_ref[...].astype(jnp.float32)
    chosen = jnp.where(
        pair < D // 8,
        place[0:1, :],
        jnp.where(pair < D // 8 + 3 * D // 16, place[1:2, :], place[2:3, :]),
    )
    angle = chosen * freq_ref[...]
    cosine = jnp.cos(angle)
    sine = jnp.sin(angle)
    cos_t[...] = jnp.concatenate([cosine, cosine], axis=0).T
    sin_t[...] = jnp.concatenate([-sine, sine], axis=0).T

    def rotate(x):
        x = x.astype(jnp.float32)
        return (x * cos_t[...] + pltpu.roll(x, HALF, 1) * sin_t[...]).astype(jnp.bfloat16)

    k_copy.wait()
    for h in range(KH):
        buf[own_slot, h, 0:ROWS, :] = rotate(kraw[:, h * D:(h + 1) * D])
    for copy in v_copies:
        copy.wait()

    query_index = own * ROWS + lax.broadcasted_iota(jnp.int32, (1, ROWS), 1)
    start = jnp.zeros((1, ROWS), jnp.int32)
    end = 0
    for d in range(8):
        length = docs_ref[d]
        end = end + length
        start = start + jnp.where(query_index >= end, length, 0)
    key_row = lax.broadcasted_iota(jnp.int32, (2 * ROWS, ROWS), 0)
    key_row = key_row + jnp.where(key_row >= ROWS, ROWS, 0)
    for pair_at in range(6):
        back, flip = pair_at // 2, pair_at % 2
        zz = 1 - z if flip else z
        key_index = key_row + (4 * (y - back) + zz) * ROWS
        allowed = (key_index >= start) & (key_index <= query_index)
        masks[pair_at] = jnp.where(allowed, BIG, LOW)

    pl.semaphore_wait(barrier, 4)

    def send(link, block, h, count):
        return pltpu.make_async_remote_copy(
            src_ref=buf.at[block, h],
            dst_ref=buf.at[block, h],
            send_sem=send_sem.at[link * 16 + count],
            recv_sem=recv_sem.at[block * 8 + h],
            device_id=links[link],
            device_id_type=MESH,
        )

    def arrived(block, h):
        pltpu.make_async_copy(
            buf.at[block, h], buf.at[block, h], recv_sem.at[block * 8 + h]
        ).wait()

    @pl.loop(0, KH)
    def _(h):
        for link in range(4):
            send(link, own_slot, h, h).start()

    acc[...] = jnp.zeros_like(acc)
    total[...] = jnp.zeros_like(total)
    best[...] = jnp.full_like(best, LOW)
    q_copy.wait()

    @pl.loop(0, KH * G)
    def _(i):
        qs[i] = rotate(qraw[:, pl.ds(pl.multiple_of(i * D, D), D)])

    def update(keys, vals, mask, h):
        scores = [
            lax.dot_general(keys, qs[h * G + g], CONTRACT_LAST, preferred_element_type=jnp.float32)
            for g in range(G)
        ]
        olds = [best[h * G + g] for g in range(G)]
        sums = [total[h * G + g] for g in range(G)]
        news, factors, parts, weights = [], [], [], []
        for g in range(G):
            sc = jnp.minimum(scores[g], mask)
            new = jnp.maximum(olds[g], jnp.max(sc, axis=0, keepdims=True))
            w = jnp.exp2(sc * EXP_SCALE - new * EXP_SCALE)
            news.append(new)
            factors.append(jnp.exp2((olds[g] - new) * EXP_SCALE))
            parts.append(jnp.sum(w, axis=0, keepdims=True))
            weights.append(w.astype(jnp.bfloat16))
        outs = [
            lax.dot_general(vals, weights[g], CONTRACT_FIRST, preferred_element_type=jnp.float32)
            for g in range(G)
        ]
        for g in range(G):
            i = h * G + g
            best[i] = news[g]
            total[i] = sums[g] * factors[g] + parts[g]
            acc[i] = acc[i] * factors[g] + outs[g]

    def needed(back, core, zz):
        block = 4 * (y - back) + 2 * core + zz
        return (block >= 0) & (block >= own - 8) & (block <= own)

    def compute(u):
        phase = lax.div(jnp.minimum(u, 15), 8)
        late = u - 8 - LAG

        @pl.loop(0, 3)
        def _(j):
            back = jnp.where(phase == 0, jnp.where(j == 1, 1, 0), jnp.where(j == 0, 1, 2))
            flip = jnp.where(phase == 0, jnp.where(j == 2, 1, 0), jnp.where(j == 1, 0, 1))
            h = jnp.where(j < 2, u - 8 * phase, jnp.where(phase == 0, u, late))
            live = jnp.where(j < 2, u < 16, (phase == 0) | ((late >= 0) & (late < 8)))
            zz = z + flip - 2 * z * flip
            first = slot(back, 0, zz)
            mask_at = back * 2 + flip
            has0 = live & needed(back, 0, zz)
            has1 = live & needed(back, 1, zz)

            @pl.when(has0 & has1)
            def _():
                both = buf[pl.ds(first, 2), h]
                update(
                    both[:, :ROWS].reshape(2 * ROWS, D),
                    both[:, ROWS:].reshape(2 * ROWS, D),
                    masks[mask_at],
                    h,
                )

            @pl.when(jnp.logical_xor(has0, has1))
            def _():
                core = jnp.where(has1, 1, 0)
                one = buf[first + core, h]
                update(
                    one[:ROWS],
                    one[ROWS:],
                    masks[mask_at, pl.ds(pl.multiple_of(core * ROWS, ROWS), ROWS)],
                    h,
                )

    def out_copy(h):
        return pltpu.make_async_copy(
            ostage.at[h], out_hbm.at[:, pl.ds(pl.multiple_of(h * G * D, D), G * D)], out_sem.at[h]
        )

    sib = 1 - c

    @pl.loop(0, 17 + LAG)
    def _(t):
        @pl.when(t < 16)
        def _():
            phase = lax.div(t, 8)
            h = lax.rem(t, 8)
            from_above = slot(3 - phase, c, z)
            arrived(from_above, h)

            @pl.when(phase == 0)
            def _():
                send(1, from_above, h, 8 + h).start()

            @pl.when(phase == 1)
            def _():
                send(2, from_above, h, 8 + h).start()
                send(3, from_above, h, 40 + h).start()

            from_below = slot(1, c, z + phase - 2 * z * phase)
            arrived(from_below, h)
            send(3, from_below, h, 8 + t).start()

        @pl.when(t < 8)
        def _():
            block = slot(0, c, 1 - z)
            arrived(block, t)
            send(0, block, t, 8 + t).start()
            send(3, block, t, 24 + t).start()

        @pl.when((t >= 8 + LAG) & (t < 16 + LAG))
        def _():
            e = t - 8 - LAG
            block = slot(2, c, 1 - z)
            arrived(block, e)
            send(3, block, e, 32 + e).start()

        u = t - 1

        @pl.when((u >= 0) & (u < 8))
        def _():
            arrived(slot(0, sib, z), u)
            arrived(slot(1, sib, z), u)
            arrived(slot(0, sib, 1 - z), u)

        @pl.when((u >= 8) & (u < 16))
        def _():
            arrived(slot(1, sib, 1 - z), u - 8)
            arrived(slot(2, sib, z), u - 8)

        @pl.when(u >= 8 + LAG)
        def _():
            arrived(slot(2, sib, 1 - z), u - 8 - LAG)

        @pl.when(u >= 0)
        def _():
            compute(u)

        @pl.when(u >= 9 + LAG)
        def _():
            out_copy(u - 9 - LAG).start()

        @pl.when(u >= 8 + LAG)
        def _():
            e = u - 8 - LAG
            for g in range(G):
                i = e * G + g
                ostage[e, :, g * D:(g + 1) * D] = (acc[i] / total[i]).T.astype(jnp.bfloat16)

    @pl.loop(0, KH)
    def _(h):
        for link in range(4):
            send(link, own_slot, h, h).wait_send()
        send(0, own_slot, h, 8 + h).wait_send()
        send(1, own_slot, h, 8 + h).wait_send()
        send(2, own_slot, h, 8 + h).wait_send()
        for more in range(5):
            send(3, own_slot, h, 8 + 8 * more + h).wait_send()

    out_copy(KH - 1).start()

    @pl.loop(0, KH)
    def _(h):
        out_copy(h).wait()


def local(queries, keys, values, positions, doc_lengths):
    exponent = -2.0 * np.arange(HALF, dtype=np.float64) / D
    freq = np.power(1000000.0, exponent).astype(np.float32)
    freq = jnp.asarray(np.broadcast_to(freq[:, None], (HALF, ROWS)))
    any_space = pl.BlockSpec(memory_space=pl.ANY)
    vmem = pl.BlockSpec(memory_space=pltpu.VMEM)
    bf16, f32 = jnp.bfloat16, jnp.float32
    heads = KH * G
    return pl.pallas_call(
        kernel,
        out_shape=jax.ShapeDtypeStruct(queries.shape, bf16),
        in_specs=[any_space, any_space, any_space, vmem, vmem, pl.BlockSpec(memory_space=pltpu.SMEM)],
        out_specs=any_space,
        scratch_shapes=[
            pltpu.VMEM((16, KH, 2 * ROWS, D), bf16),
            pltpu.VMEM((ROWS, heads * D), bf16),
            pltpu.VMEM((heads, ROWS, D), bf16),
            pltpu.VMEM((ROWS, KH * D), bf16),
            pltpu.VMEM((heads, D, ROWS), f32),
            pltpu.VMEM((heads, 1, ROWS), f32),
            pltpu.VMEM((heads, 1, ROWS), f32),
            pltpu.VMEM((6, 2 * ROWS, ROWS), f32),
            pltpu.VMEM((ROWS, D), f32),
            pltpu.VMEM((ROWS, D), f32),
            pltpu.VMEM((KH, ROWS, G * D), bf16),
            pltpu.SemaphoreType.DMA((2,)),
            pltpu.SemaphoreType.DMA((KH,)),
            pltpu.SemaphoreType.DMA((KH,)),
            pltpu.SemaphoreType.DMA((96,)),
            pltpu.SemaphoreType.DMA((128,)),
        ],
        compiler_params=pltpu.CompilerParams(
            collective_id=0, has_side_effects=True, vmem_limit_bytes=60 * 1024 * 1024
        ),
    )(queries, keys, values, positions, freq, doc_lengths)


def solution(mesh):
    rows = ("seq", "blk", "uly")
    in_specs = (P(rows, None), P(rows, None), P(rows, None), P(None, rows), P("seq"))
    return jax.shard_map(
        local, mesh=mesh, in_specs=in_specs, out_specs=P(rows, None), check_vma=False
    )
```

```python
import math

import jax
import jax.numpy as jnp
from jax import lax
from jax.experimental import pallas as pl
from jax.experimental.pallas import tpu as pltpu
from jax.sharding import PartitionSpec as P

D = 128
G = 5
KH = 8
ROWS = 256
LAG = 2
AHEAD = 5
CHUNK = 16
HALF = D // 2
BIG = 3.0e38
LOW = -1.0e30
EXP_SCALE = math.log2(math.e) / math.sqrt(D)
MESH = pl.DeviceIdType.MESH
CONTRACT_LAST = (((1,), (1,)), ((), ()))
CONTRACT_FIRST = (((0,), (0,)), ((), ()))


def kernel(
    q_hbm, k_hbm, v_hbm, pos_ref, docs_ref, out_ref,
    buf, qraw, qs, kraw, acc, best, total, held, weights, masks, bias, onehot, cos_t, sin_t,
    in_sem, v_sem, send_sem, recv_sem,
):
    s = lax.axis_index("seq")
    blk = lax.axis_index("blk")
    z = lax.axis_index("uly")
    y = lax.div(blk, 2)
    c = lax.rem(blk, 2)
    own = 4 * y + 2 * c + z
    up = (s, 2 * lax.rem(y + 1, 4) + c, z)
    down = (s, 2 * lax.rem(y + 3, 4) + c, z)
    across = (s, blk, 1 - z)
    sibling = (s, 2 * y + 1 - c, z)
    links = (up, down, across, sibling)

    def slot(back, core, zz):
        return 4 * lax.rem(y + 4 - back, 4) + 2 * zz + core

    own_slot = slot(0, c, z)

    k_copy = pltpu.make_async_copy(k_hbm, kraw, in_sem.at[0])
    k_copy.start()
    v_copies = [
        pltpu.make_async_copy(
            v_hbm.at[:, h * D:(h + 1) * D], buf.at[own_slot, h, ROWS:2 * ROWS, :], v_sem.at[h]
        )
        for h in range(KH)
    ]
    for copy in v_copies:
        copy.start()
    q_copy = pltpu.make_async_copy(q_hbm, qraw, in_sem.at[1])
    q_copy.start()

    barrier = pltpu.get_barrier_semaphore()
    for peer in links:
        pl.semaphore_signal(barrier, inc=1, device_id=peer, device_id_type=MESH)

    pair = lax.broadcasted_iota(jnp.int32, (HALF, ROWS), 0)
    place = pos_ref[...].astype(jnp.float32)
    chosen = jnp.where(
        pair < D // 8,
        place[0:1, :],
        jnp.where(pair < D // 8 + 3 * D // 16, place[1:2, :], place[2:3, :]),
    )
    step = -2.0 * math.log2(1000000.0) / D
    angle = chosen * jnp.exp2(step * pair.astype(jnp.float32))
    cosine = jnp.cos(angle)
    sine = jnp.sin(angle)
    cos_t[...] = jnp.concatenate([cosine, cosine], axis=0).T
    sin_t[...] = jnp.concatenate([-sine, sine], axis=0).T

    def rotate(x):
        x = x.astype(jnp.float32)
        return (x * cos_t[...] + pltpu.roll(x, HALF, 1) * sin_t[...]).astype(jnp.bfloat16)

    k_copy.wait()
    for h in range(KH):
        buf[own_slot, h, 0:ROWS, :] = rotate(kraw[:, h * D:(h + 1) * D])
    for copy in v_copies:
        copy.wait()

    pl.semaphore_wait(barrier, 4)

    def send(link, block, h, count):
        return pltpu.make_async_remote_copy(
            src_ref=buf.at[block, h],
            dst_ref=buf.at[block, h],
            send_sem=send_sem.at[link * 16 + count],
            recv_sem=recv_sem.at[block * 8 + h],
            device_id=links[link],
            device_id_type=MESH,
        )

    def arrived(block, h):
        pltpu.make_async_copy(
            buf.at[block, h], buf.at[block, h], recv_sem.at[block * 8 + h]
        ).wait()

    @pl.loop(0, KH)
    def _(h):
        for link in range(4):
            send(link, own_slot, h, h).start()

    lane = lax.broadcasted_iota(jnp.int32, (1, D), 1)
    first_of = jnp.zeros((1, D), jnp.int32)
    end_of = jnp.zeros((1, D), jnp.int32)
    end = 0
    for d in range(8):
        first_of = jnp.where(lane == d, end, first_of)
        end = end + docs_ref[d]
        end_of = jnp.where(lane == d, end, end_of)
    row = lax.broadcasted_iota(jnp.int32, (ROWS, D), 0)
    index = row + own * ROWS
    inside = (index >= first_of) & (index < end_of)
    onehot[...] = jnp.where(inside, 1.0, 0.0).astype(jnp.bfloat16)
    for at in range(12):
        back, flip, core = at // 4, at // 2 % 2, at % 2
        zz = 1 - z if flip else z
        index = row + (4 * (y - back) + 2 * core + zz) * ROWS
        inside = ((index >= first_of) & (index < end_of)) | (lane >= 8)
        bias[at] = jnp.where(inside, 0.0, LOW).astype(jnp.bfloat16)
    key_row = lax.broadcasted_iota(jnp.int32, (ROWS, ROWS), 0)
    query_row = lax.broadcasted_iota(jnp.int32, (ROWS, ROWS), 1)
    masks[0] = jnp.where(key_row <= query_row, BIG, LOW)
    masks[1] = jnp.full((ROWS, ROWS), BIG, jnp.float32)

    acc[...] = jnp.zeros_like(acc)
    total[...] = jnp.zeros_like(total)
    best[...] = jnp.full_like(best, LOW)
    q_copy.wait()

    @pl.loop(0, KH * G)
    def _(i):
        qs[i] = rotate(qraw[:, pl.ds(pl.multiple_of(i * D, D), D)])

    def update(places, bias_at, phase, h):
        width = len(places) * ROWS
        keys = jnp.concatenate(
            [
                jnp.concatenate([buf[p, h, :ROWS, :], bias[at]], axis=1)
                for p, at in zip(places, bias_at)
            ],
            axis=0,
        )
        vals = jnp.concatenate([buf[p, h, ROWS:, :] for p in places], axis=0)
        olds = [best[h * G + g] for g in range(G)]
        sums = [total[h * G + g] for g in range(G)]
        news, factors, parts, outs = [], [], [], []

        def score(g):
            query = jnp.concatenate([qs[h * G + g], onehot[...]], axis=1)
            sc = lax.dot_general(keys, query, CONTRACT_LAST, preferred_element_type=jnp.float32)
            head = jnp.minimum(sc[:ROWS], masks[phase])
            held[g, :ROWS] = head
            held[g, ROWS:width] = sc[ROWS:]
            new = jnp.maximum(olds[g], jnp.max(head, axis=0, keepdims=True))
            new = jnp.maximum(new, jnp.max(sc[ROWS:], axis=0, keepdims=True))
            news.append(new)
            factors.append(jnp.exp2((olds[g] - new) * EXP_SCALE))

        def soften(g):
            level = news[g] * EXP_SCALE
            part = jnp.zeros((8, ROWS), jnp.float32)
            for at in range(0, width, CHUNK):
                w = jnp.exp2(held[g, at:at + CHUNK] * EXP_SCALE - level)
                for row in range(0, CHUNK, 8):
                    part = part + w[row:row + 8]
                weights[g, at:at + CHUNK] = w.astype(jnp.bfloat16)
            parts.append(jnp.sum(part, axis=0, keepdims=True))

        def gather(g):
            outs.append(
                lax.dot_general(
                    vals, weights[g, :width], CONTRACT_FIRST, preferred_element_type=jnp.float32
                )
            )

        for g in range(AHEAD):
            score(g)
        for g in range(G):
            if g + AHEAD < G:
                score(g + AHEAD)
            soften(g)
            gather(g)
        for g in range(G):
            i = h * G + g
            best[i] = news[g]
            total[i] = sums[g] * factors[g] + parts[g]
            acc[i] = acc[i] * factors[g] + outs[g]

    rank = 2 * c + z

    def early_blocks(r):
        blocks = [(0, 0, r // 2), (1, 0, 0), (1, 0, 1)]
        for core in range(2):
            for flip in range(2):
                if 2 * core + ((r % 2) ^ flip) < r:
                    blocks.append((0, flip, core))
        return blocks

    def late_blocks(r):
        blocks = [(1, 1, 0), (1, 1, 1)]
        for flip in range(2):
            for core in range(2):
                if 2 * core + ((r % 2) ^ flip) >= r:
                    blocks.append((2, flip, core))
        return blocks

    def compute(phase, h):
        for count in range(3, 7):
            early, late = early_blocks(count - 3), late_blocks(6 - count)
            assert len(early) == count and len(late) == count

            @pl.when(rank == jnp.where(phase == 0, count - 3, 6 - count))
            def _():
                def place(b):
                    back, flip, core = b
                    return slot(back, core, 1 - z if flip else z)

                def bias_of(b):
                    return 4 * b[0] + 2 * b[1] + b[2]

                update(
                    [jnp.where(phase == 0, place(e), place(f)) for e, f in zip(early, late)],
                    [jnp.where(phase == 0, bias_of(e), bias_of(f)) for e, f in zip(early, late)],
                    phase,
                    h,
                )

    sib = 1 - c

    @pl.loop(0, 17 + LAG)
    def _(t):
        @pl.when(t < 16)
        def _():
            phase = lax.div(t, 8)
            h = lax.rem(t, 8)
            from_above = slot(3 - phase, c, z)
            arrived(from_above, h)

            @pl.when(phase == 0)
            def _():
                send(1, from_above, h, 8 + h).start()

            @pl.when(phase == 1)
            def _():
                send(2, from_above, h, 8 + h).start()
                send(3, from_above, h, 40 + h).start()

            from_below = slot(1, c, z + phase - 2 * z * phase)
            arrived(from_below, h)
            send(3, from_below, h, 8 + t).start()

        @pl.when(t < 8)
        def _():
            block = slot(0, c, 1 - z)
            arrived(block, t)
            send(0, block, t, 8 + t).start()
            send(3, block, t, 24 + t).start()

        @pl.when((t >= 8 + LAG) & (t < 16 + LAG))
        def _():
            e = t - 8 - LAG
            block = slot(2, c, 1 - z)
            arrived(block, e)
            send(3, block, e, 32 + e).start()

        u = t - 1

        @pl.when((u >= 0) & (u < 8))
        def _():
            arrived(slot(0, sib, z), u)
            arrived(slot(1, sib, z), u)
            arrived(slot(0, sib, 1 - z), u)

        @pl.when((u >= 8) & (u < 16))
        def _():
            arrived(slot(1, sib, 1 - z), u - 8)
            arrived(slot(2, sib, z), u - 8)

        @pl.when(u >= 8 + LAG)
        def _():
            arrived(slot(2, sib, 1 - z), u - 8 - LAG)

        late = u - 8 - LAG

        @pl.when(((u >= 0) & (u < 8)) | (late >= 0))
        def _():
            compute(jnp.where(late >= 0, 1, 0), jnp.where(late >= 0, late, u))

        @pl.when(u >= 8 + LAG)
        def _():
            e = u - 8 - LAG
            for g in range(G):
                i = e * G + g
                out_ref[:, pl.ds(pl.multiple_of(i * D, D), D)] = (
                    (acc[i] / total[i]).T.astype(jnp.bfloat16)
                )

    @pl.loop(0, KH)
    def _(h):
        for link in range(4):
            send(link, own_slot, h, h).wait_send()
        send(0, own_slot, h, 8 + h).wait_send()
        send(1, own_slot, h, 8 + h).wait_send()
        send(2, own_slot, h, 8 + h).wait_send()
        for more in range(5):
            send(3, own_slot, h, 8 + 8 * more + h).wait_send()


def local(queries, keys, values, positions, doc_lengths):
    any_space = pl.BlockSpec(memory_space=pl.ANY)
    vmem = pl.BlockSpec(memory_space=pltpu.VMEM)
    bf16, f32 = jnp.bfloat16, jnp.float32
    heads = KH * G
    return pl.pallas_call(
        kernel,
        out_shape=pltpu.VMEM(queries.shape, bf16),
        in_specs=[any_space, any_space, any_space, vmem, pl.BlockSpec(memory_space=pltpu.SMEM)],
        out_specs=vmem,
        scratch_shapes=[
            pltpu.VMEM((16, KH, 2 * ROWS, D), bf16),
            pltpu.VMEM((ROWS, heads * D), bf16),
            pltpu.VMEM((heads, ROWS, D), bf16),
            pltpu.VMEM((ROWS, KH * D), bf16),
            pltpu.VMEM((heads, D, ROWS), f32),
            pltpu.VMEM((heads, 1, ROWS), f32),
            pltpu.VMEM((heads, 1, ROWS), f32),
            pltpu.VMEM((G, 6 * ROWS, ROWS), f32),
            pltpu.VMEM((G, 6 * ROWS, ROWS), bf16),
            pltpu.VMEM((2, ROWS, ROWS), f32),
            pltpu.VMEM((12, ROWS, D), bf16),
            pltpu.VMEM((ROWS, D), bf16),
            pltpu.VMEM((ROWS, D), f32),
            pltpu.VMEM((ROWS, D), f32),
            pltpu.SemaphoreType.DMA((2,)),
            pltpu.SemaphoreType.DMA((KH,)),
            pltpu.SemaphoreType.DMA((96,)),
            pltpu.SemaphoreType.DMA((128,)),
        ],
        compiler_params=pltpu.CompilerParams(
            collective_id=0, has_side_effects=True, vmem_limit_bytes=56 * 1024 * 1024
        ),
    )(queries, keys, values, positions, doc_lengths)


def solution(mesh):
    rows = ("seq", "blk", "uly")
    in_specs = (P(rows, None), P(rows, None), P(rows, None), P(None, rows), P("seq"))
    return jax.shard_map(
        local, mesh=mesh, in_specs=in_specs, out_specs=P(rows, None), check_vma=False
    )
```

```python
import math

import jax
import jax.numpy as jnp
from jax import lax
from jax.experimental import pallas as pl
from jax.experimental.pallas import tpu as pltpu
from jax.sharding import PartitionSpec as P

D = 128
G = 5
KH = 8
ROWS = 256
UP, DOWN, ACROSS, SIBLING = range(4)
LATE = 11
AHEAD = 5
CHUNK = 16
HALF = D // 2
BIG = 3.0e38
LOW = -1.0e30
EXP_SCALE = math.log2(math.e) / math.sqrt(D)
MESH = pl.DeviceIdType.MESH
CONTRACT_LAST = (((1,), (1,)), ((), ()))
CONTRACT_FIRST = (((0,), (0,)), ((), ()))


def kernel(
    q_hbm, k_hbm, v_hbm, pos_ref, docs_ref, out_ref,
    buf, qraw, qs, kraw, acc, best, total, held, weights, masks, bias, onehot, cos_t, sin_t,
    in_sem, v_sem, send_sem, recv_sem,
):
    s = lax.axis_index("seq")
    blk = lax.axis_index("blk")
    z = lax.axis_index("uly")
    y = lax.div(blk, 2)
    c = lax.rem(blk, 2)
    own = 4 * y + 2 * c + z
    up = (s, 2 * lax.rem(y + 1, 4) + c, z)
    down = (s, 2 * lax.rem(y + 3, 4) + c, z)
    across = (s, blk, 1 - z)
    sibling = (s, 2 * y + 1 - c, z)
    links = (up, down, across, sibling)

    def slot(back, core, zz):
        return 4 * lax.rem(y + 4 - back, 4) + 2 * zz + core

    own_slot = slot(0, c, z)

    k_copy = pltpu.make_async_copy(k_hbm, kraw, in_sem.at[0])
    k_copy.start()
    v_copies = [
        pltpu.make_async_copy(
            v_hbm.at[:, h * D:(h + 1) * D], buf.at[own_slot * KH + h, ROWS:2 * ROWS, :], v_sem.at[h]
        )
        for h in range(KH)
    ]
    for copy in v_copies:
        copy.start()
    q_copy = pltpu.make_async_copy(q_hbm, qraw, in_sem.at[1])
    q_copy.start()

    barrier = pltpu.get_barrier_semaphore()
    for peer in links:
        pl.semaphore_signal(barrier, inc=1, device_id=peer, device_id_type=MESH)

    pair = lax.broadcasted_iota(jnp.int32, (HALF, ROWS), 0)
    place = pos_ref[...].astype(jnp.float32)
    chosen = jnp.where(
        pair < D // 8,
        place[0:1, :],
        jnp.where(pair < D // 8 + 3 * D // 16, place[1:2, :], place[2:3, :]),
    )
    step = -2.0 * math.log2(1000000.0) / D
    angle = chosen * jnp.exp2(step * pair.astype(jnp.float32))
    cosine = jnp.cos(angle)
    sine = jnp.sin(angle)
    cos_t[...] = jnp.concatenate([cosine, cosine], axis=0).T
    sin_t[...] = jnp.concatenate([-sine, sine], axis=0).T

    def rotate(x):
        x = x.astype(jnp.float32)
        return (x * cos_t[...] + pltpu.roll(x, HALF, 1) * sin_t[...]).astype(jnp.bfloat16)

    k_copy.wait()
    for h in range(KH):
        buf[own_slot * KH + h, 0:ROWS, :] = rotate(kraw[:, h * D:(h + 1) * D])
    for copy in v_copies:
        copy.wait()

    pl.semaphore_wait(barrier, 4)

    def send(link, block, h, sem=None):
        at = block * KH + h
        pltpu.make_async_remote_copy(
            src_ref=buf.at[at],
            dst_ref=buf.at[at],
            send_sem=send_sem.at[link if sem is None else sem],
            recv_sem=recv_sem.at[at],
            device_id=links[link],
            device_id_type=MESH,
        ).start()

    def arrived(block, h):
        at = block * KH + h
        pltpu.make_async_copy(buf.at[at], buf.at[at], recv_sem.at[at]).wait()

    def sent(sem, count):
        if count:
            some = buf.at[pl.ds(0, count)]
            pltpu.make_async_copy(some, some, send_sem.at[sem]).wait()

    gives_own = jnp.logical_not((c == 1) & (z == 1))
    takes_own = jnp.logical_not((c == 1) & (z == 0))
    sib_takes_own = jnp.logical_not((c == 0) & (z == 0))
    gives_far = jnp.logical_not((c == 0) & (z == 0))
    takes_far = jnp.logical_not((c == 0) & (z == 1))
    sib_takes_far = jnp.logical_not((c == 1) & (z == 1))

    @pl.loop(0, KH)
    def _(h):
        @pl.when((y == 0) | (y == 2) | ((y == 1) & (h < 2)))
        def _():
            send(UP, own_slot, h)

        @pl.when(((y == 0) & (h < 6)) | (y == 1))
        def _():
            send(DOWN, own_slot, h)

        @pl.when(y < 3)
        def _():
            send(ACROSS, own_slot, h)

        @pl.when((y == 3) & gives_own)
        def _():
            send(ACROSS, own_slot, h, 4)

        send(SIBLING, own_slot, h)

    lane = lax.broadcasted_iota(jnp.int32, (1, D), 1)
    first_of = jnp.zeros((1, D), jnp.int32)
    end_of = jnp.zeros((1, D), jnp.int32)
    end = 0
    for d in range(8):
        first_of = jnp.where(lane == d, end, first_of)
        end = end + docs_ref[d]
        end_of = jnp.where(lane == d, end, end_of)
    row = lax.broadcasted_iota(jnp.int32, (ROWS, D), 0)
    index = row + own * ROWS
    inside = (index >= first_of) & (index < end_of)
    onehot[...] = jnp.where(inside, 1.0, 0.0).astype(jnp.bfloat16)
    for at in range(12):
        back, flip, core = at // 4, at // 2 % 2, at % 2
        zz = 1 - z if flip else z
        index = row + (4 * (y - back) + 2 * core + zz) * ROWS
        inside = ((index >= first_of) & (index < end_of)) | (lane >= 8)
        bias[at] = jnp.where(inside, 0.0, LOW).astype(jnp.bfloat16)
    bias[12] = jnp.where(row * 0 + lane < 8, LOW, 0.0).astype(jnp.bfloat16)
    key_row = lax.broadcasted_iota(jnp.int32, (ROWS, ROWS), 0)
    query_row = lax.broadcasted_iota(jnp.int32, (ROWS, ROWS), 1)
    masks[0] = jnp.where(key_row <= query_row, BIG, LOW)
    masks[1] = jnp.full((ROWS, ROWS), BIG, jnp.float32)

    acc[...] = jnp.zeros_like(acc)
    total[...] = jnp.zeros_like(total)
    best[...] = jnp.full_like(best, LOW)
    q_copy.wait()

    @pl.loop(0, KH * G)
    def _(i):
        qs[i] = rotate(qraw[:, pl.ds(pl.multiple_of(i * D, D), D)])

    def update(places, bias_at, phase, h):
        width = len(places) * ROWS
        keys = jnp.concatenate(
            [
                jnp.concatenate([buf[p * KH + h, :ROWS, :], bias[at]], axis=1)
                for p, at in zip(places, bias_at)
            ],
            axis=0,
        )
        vals = jnp.concatenate([buf[p * KH + h, ROWS:, :] for p in places], axis=0)
        olds = [best[h * G + g] for g in range(G)]
        sums = [total[h * G + g] for g in range(G)]
        news, factors, parts, outs = [], [], [], []

        def score(g):
            query = jnp.concatenate([qs[h * G + g], onehot[...]], axis=1)
            sc = lax.dot_general(keys, query, CONTRACT_LAST, preferred_element_type=jnp.float32)
            head = jnp.minimum(sc[:ROWS], masks[phase])
            held[g, :ROWS] = head
            held[g, ROWS:width] = sc[ROWS:]
            new = jnp.maximum(olds[g], jnp.max(head, axis=0, keepdims=True))
            new = jnp.maximum(new, jnp.max(sc[ROWS:], axis=0, keepdims=True))
            news.append(new)
            factors.append(jnp.exp2((olds[g] - new) * EXP_SCALE))

        def soften(g):
            level = news[g] * EXP_SCALE
            part = jnp.zeros((8, ROWS), jnp.float32)
            for at in range(0, width, CHUNK):
                w = jnp.exp2(held[g, at:at + CHUNK] * EXP_SCALE - level)
                for row in range(0, CHUNK, 8):
                    part = part + w[row:row + 8]
                weights[g, at:at + CHUNK] = w.astype(jnp.bfloat16)
            parts.append(jnp.sum(part, axis=0, keepdims=True))

        def gather(g):
            outs.append(
                lax.dot_general(
                    vals, weights[g, :width], CONTRACT_FIRST, preferred_element_type=jnp.float32
                )
            )

        for g in range(AHEAD):
            score(g)
        for g in range(G):
            if g + AHEAD < G:
                score(g + AHEAD)
            soften(g)
            gather(g)
        for g in range(G):
            i = h * G + g
            best[i] = news[g]
            total[i] = sums[g] * factors[g] + parts[g]
            acc[i] = acc[i] * factors[g] + outs[g]

    rank = 2 * c + z

    def block_lists(k, r):
        near = [(0, 0, r // 2)] + [
            (0, flip, core) for core in range(2) for flip in range(2) if 2 * core + ((r % 2) ^ flip) < r
        ]
        same, cross = [(1, 0, 0), (1, 0, 1)], [(1, 1, 0), (1, 1, 1)]
        far = [(2, 0, core) for core in range(2) if 2 * core + r % 2 >= r]
        far_cross = [(2, 1, core) for core in range(2) if 2 * core + 1 - r % 2 >= r]
        if k == 0:
            first, second = near, []
        elif k == 2:
            spare = 2 - min(r, 2)
            first = near + cross[: 1 if r == 3 else 2] + far[:spare]
            second = (cross[1:] if r == 3 else []) + same + far[spare:] + far_cross
        else:
            first = near + same[: 1 if r == 3 else 2]
            second = (same[1:] if r == 3 else []) + cross + (far + far_cross if k == 3 else [])
        pad = [(k + 1, 0, 0)] * 3
        first = first + pad[: max(0, 3 - len(first))]
        second = second + (pad[: max(0, 3 - len(second))] if second else [])
        return first, second

    lists = {(k, r): block_lists(k, r) for k in range(4) for r in range(4)}

    def chosen_by_place(value):
        result = 0
        for (k, r), pair in lists.items():
            result = jnp.where((y == k) & (rank == r), value(pair), result)
        return result

    def resolve(phase, at):
        def field(n):
            return chosen_by_place(lambda pair: (pair[phase] + [(3, 0, 0)] * 6)[at][n])

        back, flip, core = field(0), field(1), field(2)
        place = slot(jnp.minimum(back, 3), core, z + flip - 2 * z * flip)
        masked = back > y
        at_bias = jnp.where(masked, 12, 4 * jnp.minimum(back, 2) + 2 * flip + core)
        return jnp.where(masked, own_slot, place), at_bias

    sizes = [chosen_by_place(lambda pair, phase=phase: len(pair[phase])) for phase in range(2)]
    resolved = [[resolve(phase, at) for at in range(6)] for phase in range(2)]

    def compute(phase, h):
        size = jnp.where(phase == 0, sizes[0], sizes[1])
        for count in range(3, 7):
            @pl.when(size == count)
            def _():
                update(
                    [jnp.where(phase == 0, resolved[0][at][0], resolved[1][at][0]) for at in range(count)],
                    [jnp.where(phase == 0, resolved[0][at][1], resolved[1][at][1]) for at in range(count)],
                    phase,
                    h,
                )

    sib = 1 - c

    def block(at_y, core, zz):
        return 4 * at_y + 2 * zz + core

    def on(condition, h, source, *onward):
        @pl.when(condition)
        def _():
            arrived(source, h)
            for link, ok, sem in onward:
                if ok is True:
                    send(link, source, h, sem)
                else:
                    @pl.when(ok)
                    def _(link=link, sem=sem):
                        send(link, source, h, sem)

    other = 1 - z
    home = [block(k, c, z) for k in range(4)]
    away = [block(k, c, other) for k in range(4)]
    sib_home = [block(k, sib, z) for k in range(4)]
    sib_away = [block(k, sib, other) for k in range(4)]
    to_sib = (SIBLING, True, None)

    def within(t, low, high):
        return (t >= low) & (t < high)

    def serve_0(t):
        on(t < 8, t, away[0], (UP, t < 6, None), to_sib)
        on(t < 8, t, home[1], (DOWN, True, None))

    def serve_1(t):
        on(t < 8, t, away[1], (UP, True, None), to_sib)
        on(t < 8, t, home[0], (UP, t >= 6, None), (ACROSS, t >= 6, None), to_sib)
        on(within(t, 8, 14), t - 8, away[0], to_sib)
        on(within(t, 10, 12), t - 4, away[0], (UP, True, None), to_sib)

    def serve_2(t):
        on(t < 8, t, away[2], (UP, t < 6, None), to_sib)
        on(t < 2, t, home[1], to_sib)
        on(within(t, 2, 8), t - 2, home[0], (ACROSS, True, None), to_sib)
        on(within(t, 2, 10), t - 2, away[1], to_sib)
        on(within(t, 10, 12), t - 4, home[0], to_sib)
        on(within(t, 9, 15), t - 9, away[0], to_sib)
        on(within(t, 10, 16), t - 8, home[1], to_sib)
        on(within(t, 12, 14), t - 6, away[0], to_sib)

    def serve_3(t):
        on(within(t, 1, 7), t - 1, home[0], (DOWN, True, None))
        on(
            within(t, 7, 15), t - 7, home[1],
            (DOWN, t >= 9, None), (ACROSS, gives_far, 5), to_sib,
        )
        on(t < 8, t, home[2], (ACROSS, t >= 6, None), to_sib)
        on((t < 8) & takes_own, t, away[3], (SIBLING, True, 6))
        on(within(t, 8, 14), t - 8, away[2], to_sib)
        on(within(t, 9, 11), t - 3, away[2], to_sib)
        on(within(t, 10, 18) & takes_far, t - 10, away[1], (SIBLING, True, 7))

    def early_0(h):
        arrived(sib_away[0], h)

    def early_1(h):
        arrived(sib_away[1], h)
        arrived(sib_home[0], h)

    def early_2(h):
        arrived(sib_away[2], h)
        arrived(sib_away[1], h)
        arrived(sib_home[0], h)

    def early_3(h):
        on(sib_takes_own, h, sib_away[3])
        arrived(sib_home[2], h)

    def late_0(h):
        pass

    def late_1(h):
        arrived(sib_away[0], h)

    def late_2(h):
        arrived(sib_home[1], h)
        arrived(sib_away[0], h)

    def late_3(h):
        arrived(sib_away[2], h)
        arrived(sib_home[1], h)
        on(sib_takes_far, h, sib_away[1])

    late_after = jnp.where(y == 3, LATE, LATE - 1)

    @pl.loop(0, 8 + LATE)
    def _(t):
        for k, serve in enumerate((serve_0, serve_1, serve_2, serve_3)):
            @pl.when(y == k)
            def _(serve=serve):
                serve(t)

        early_h = jnp.where(y == 2, jnp.where(t < 10, t - 3, t - 5), t - 1)
        late_h = t - late_after
        early = jnp.where(y == 2, within(t, 3, 9) | within(t, 11, 13), within(t, 1, 9))
        late = within(late_h, 0, 8)

        @pl.when(early)
        def _():
            arrived(slot(0, sib, z), early_h)
            for k, wait in enumerate((early_0, early_1, early_2, early_3)):
                @pl.when(y == k)
                def _(wait=wait):
                    wait(early_h)

        @pl.when(late)
        def _():
            for k, wait in enumerate((late_0, late_1, late_2, late_3)):
                @pl.when(y == k)
                def _(wait=wait):
                    wait(late_h)

        @pl.loop(0, 2)
        def _(phase):
            @pl.when(jnp.where(phase == 0, early, late))
            def _():
                compute(phase, jnp.where(phase == 0, early_h, late_h))

        @pl.when(late)
        def _():
            for g in range(G):
                i = late_h * G + g
                out_ref[:, pl.ds(pl.multiple_of(i * D, D), D)] = (
                    (acc[i] / total[i]).T.astype(jnp.bfloat16)
                )

    counts = ((14, 14, 8, 16), (14, 8, 10, 32), (14, 0, 14, 48), (0, 12, 2, 32))
    for k in range(4):
        @pl.when(y == k)
        def _(k=k):
            for link in range(4):
                sent(link, counts[k][link])

    @pl.when(y == 3)
    def _():
        for sem, used in ((4, gives_own), (5, gives_far), (6, takes_own), (7, takes_far)):
            @pl.when(used)
            def _(sem=sem):
                sent(sem, KH)


def local(queries, keys, values, positions, doc_lengths):
    any_space = pl.BlockSpec(memory_space=pl.ANY)
    vmem = pl.BlockSpec(memory_space=pltpu.VMEM)
    bf16, f32 = jnp.bfloat16, jnp.float32
    heads = KH * G
    return pl.pallas_call(
        kernel,
        out_shape=pltpu.VMEM(queries.shape, bf16),
        in_specs=[any_space, any_space, any_space, vmem, pl.BlockSpec(memory_space=pltpu.SMEM)],
        out_specs=vmem,
        scratch_shapes=[
            pltpu.VMEM((16 * KH, 2 * ROWS, D), bf16),
            pltpu.VMEM((ROWS, heads * D), bf16),
            pltpu.VMEM((heads, ROWS, D), bf16),
            pltpu.VMEM((ROWS, KH * D), bf16),
            pltpu.VMEM((heads, D, ROWS), f32),
            pltpu.VMEM((heads, 1, ROWS), f32),
            pltpu.VMEM((heads, 1, ROWS), f32),
            pltpu.VMEM((G, 6 * ROWS, ROWS), f32),
            pltpu.VMEM((G, 6 * ROWS, ROWS), bf16),
            pltpu.VMEM((2, ROWS, ROWS), f32),
            pltpu.VMEM((13, ROWS, D), bf16),
            pltpu.VMEM((ROWS, D), bf16),
            pltpu.VMEM((ROWS, D), f32),
            pltpu.VMEM((ROWS, D), f32),
            pltpu.SemaphoreType.DMA((2,)),
            pltpu.SemaphoreType.DMA((KH,)),
            pltpu.SemaphoreType.DMA((8,)),
            pltpu.SemaphoreType.DMA((128,)),
        ],
        compiler_params=pltpu.CompilerParams(
            collective_id=0, has_side_effects=True, vmem_limit_bytes=56 * 1024 * 1024
        ),
    )(queries, keys, values, positions, doc_lengths)


def solution(mesh):
    rows = ("seq", "blk", "uly")
    in_specs = (P(rows, None), P(rows, None), P(rows, None), P(None, rows), P("seq"))
    return jax.shard_map(
        local, mesh=mesh, in_specs=in_specs, out_specs=P(rows, None), check_vma=False
    )
```

```python
import math

import jax
import jax.numpy as jnp
from jax import lax
from jax.experimental import pallas as pl
from jax.experimental.pallas import tpu as pltpu
from jax.sharding import PartitionSpec as P

D = 128
G = 5
KH = 8
ROWS = 256
UP, DOWN, ACROSS, SIBLING = range(4)
LATE = 11
AHEAD = 5
CHUNK = 16
HALF = D // 2
BIG = 3.0e38
LOW = -1.0e30
EXP_SCALE = math.log2(math.e) / math.sqrt(D)
MESH = pl.DeviceIdType.MESH
CONTRACT_LAST = (((1,), (1,)), ((), ()))
CONTRACT_FIRST = (((0,), (0,)), ((), ()))


def kernel(
    q_hbm, k_hbm, v_hbm, pos_ref, docs_ref, out_ref,
    buf, qraw, qs, kraw, acc, best, total, held, weights, masks, bias, onehot, cos_t, sin_t,
    in_sem, v_sem, send_sem, recv_sem,
):
    s = lax.axis_index("seq")
    blk = lax.axis_index("blk")
    z = lax.axis_index("uly")
    y = lax.div(blk, 2)
    c = lax.rem(blk, 2)
    own = 4 * y + 2 * c + z
    up = (s, 2 * lax.rem(y + 1, 4) + c, z)
    down = (s, 2 * lax.rem(y + 3, 4) + c, z)
    across = (s, blk, 1 - z)
    sibling = (s, 2 * y + 1 - c, z)
    links = (up, down, across, sibling)

    def slot(back, core, zz):
        return 4 * lax.rem(y + 4 - back, 4) + 2 * zz + core

    own_slot = slot(0, c, z)

    k_copy = pltpu.make_async_copy(k_hbm, kraw, in_sem.at[0])
    k_copy.start()
    v_copies = [
        pltpu.make_async_copy(
            v_hbm.at[:, h * D:(h + 1) * D], buf.at[own_slot * KH + h, ROWS:2 * ROWS, :], v_sem.at[h]
        )
        for h in range(KH)
    ]
    for copy in v_copies:
        copy.start()
    q_copy = pltpu.make_async_copy(q_hbm, qraw, in_sem.at[1])
    q_copy.start()

    barrier = pltpu.get_barrier_semaphore()
    for peer in links:
        pl.semaphore_signal(barrier, inc=1, device_id=peer, device_id_type=MESH)

    def send_part(h, low):
        at = own_slot * KH + h
        for link, ok, sem in ((UP, y < 3, 0), (DOWN, y < 2, 1), (ACROSS, y < 3, 2), (SIBLING, y < 4, 3)):
            @pl.when(ok)
            def _(link=link, sem=sem):
                pltpu.make_async_remote_copy(
                    src_ref=buf.at[at, low:low + ROWS, :],
                    dst_ref=buf.at[at, low:low + ROWS, :],
                    send_sem=send_sem.at[sem],
                    recv_sem=recv_sem.at[at],
                    device_id=links[link],
                    device_id_type=MESH,
                ).start()

    for copy in v_copies:
        copy.wait()
    pl.semaphore_wait(barrier, 4)
    for h in range(2):
        send_part(h, ROWS)

    pair = lax.broadcasted_iota(jnp.int32, (HALF, ROWS), 0)
    place = pos_ref[...].astype(jnp.float32)
    chosen = jnp.where(
        pair < D // 8,
        place[0:1, :],
        jnp.where(pair < D // 8 + 3 * D // 16, place[1:2, :], place[2:3, :]),
    )
    step = -2.0 * math.log2(1000000.0) / D
    angle = chosen * jnp.exp2(step * pair.astype(jnp.float32))
    cosine = jnp.cos(angle)
    sine = jnp.sin(angle)
    cos_t[...] = jnp.concatenate([cosine, cosine], axis=0).T
    sin_t[...] = jnp.concatenate([-sine, sine], axis=0).T

    def rotate(x):
        x = x.astype(jnp.float32)
        return (x * cos_t[...] + pltpu.roll(x, HALF, 1) * sin_t[...]).astype(jnp.bfloat16)

    k_copy.wait()
    for h in range(KH):
        buf[own_slot * KH + h, 0:ROWS, :] = rotate(kraw[:, h * D:(h + 1) * D])

    def send(link, block, h, sem=None):
        at = block * KH + h
        pltpu.make_async_remote_copy(
            src_ref=buf.at[at],
            dst_ref=buf.at[at],
            send_sem=send_sem.at[link if sem is None else sem],
            recv_sem=recv_sem.at[at],
            device_id=links[link],
            device_id_type=MESH,
        ).start()

    def arrived(block, h):
        at = block * KH + h
        pltpu.make_async_copy(buf.at[at], buf.at[at], recv_sem.at[at]).wait()

    def sent(sem, count):
        if count:
            some = buf.at[pl.ds(0, count)]
            pltpu.make_async_copy(some, some, send_sem.at[sem]).wait()

    gives_own = jnp.logical_not((c == 1) & (z == 1))
    takes_own = jnp.logical_not((c == 1) & (z == 0))
    sib_takes_own = jnp.logical_not((c == 0) & (z == 0))
    gives_far = jnp.logical_not((c == 0) & (z == 0))
    takes_far = jnp.logical_not((c == 0) & (z == 1))
    sib_takes_far = jnp.logical_not((c == 1) & (z == 1))

    for h in range(2):
        send_part(h, 0)

    @pl.when((y == 3) & gives_own)
    def _():
        for h in range(2):
            send(ACROSS, own_slot, h, 4)

    @pl.loop(2, KH)
    def _(h):
        @pl.when((y == 0) | (y == 2))
        def _():
            send(UP, own_slot, h)

        @pl.when(((y == 0) & (h < 6)) | (y == 1))
        def _():
            send(DOWN, own_slot, h)

        @pl.when(y < 3)
        def _():
            send(ACROSS, own_slot, h)

        @pl.when((y == 3) & gives_own)
        def _():
            send(ACROSS, own_slot, h, 4)

        send(SIBLING, own_slot, h)

    lane = lax.broadcasted_iota(jnp.int32, (1, D), 1)
    first_of = jnp.zeros((1, D), jnp.int32)
    end_of = jnp.zeros((1, D), jnp.int32)
    end = 0
    for d in range(8):
        first_of = jnp.where(lane == d, end, first_of)
        end = end + docs_ref[d]
        end_of = jnp.where(lane == d, end, end_of)
    row = lax.broadcasted_iota(jnp.int32, (ROWS, D), 0)
    index = row + own * ROWS
    inside = (index >= first_of) & (index < end_of)
    onehot[...] = jnp.where(inside, 1.0, 0.0).astype(jnp.bfloat16)
    for at in range(12):
        back, flip, core = at // 4, at // 2 % 2, at % 2
        zz = 1 - z if flip else z
        index = row + (4 * (y - back) + 2 * core + zz) * ROWS
        inside = ((index >= first_of) & (index < end_of)) | (lane >= 8)
        bias[at] = jnp.where(inside, 0.0, LOW).astype(jnp.bfloat16)
    bias[12] = jnp.where(row * 0 + lane < 8, LOW, 0.0).astype(jnp.bfloat16)
    key_row = lax.broadcasted_iota(jnp.int32, (ROWS, ROWS), 0)
    query_row = lax.broadcasted_iota(jnp.int32, (ROWS, ROWS), 1)
    masks[0] = jnp.where(key_row <= query_row, BIG, LOW)
    masks[1] = jnp.full((ROWS, ROWS), BIG, jnp.float32)

    acc[...] = jnp.zeros_like(acc)
    total[...] = jnp.zeros_like(total)
    best[...] = jnp.full_like(best, LOW)
    q_copy.wait()

    @pl.loop(0, KH * G)
    def _(i):
        qs[i] = rotate(qraw[:, pl.ds(pl.multiple_of(i * D, D), D)])

    def update(places, bias_at, phase, h):
        width = len(places) * ROWS
        keys = jnp.concatenate(
            [
                jnp.concatenate([buf[p * KH + h, :ROWS, :], bias[at]], axis=1)
                for p, at in zip(places, bias_at)
            ],
            axis=0,
        )
        vals = jnp.concatenate([buf[p * KH + h, ROWS:, :] for p in places], axis=0)
        olds = [best[h * G + g] for g in range(G)]
        sums = [total[h * G + g] for g in range(G)]
        news, factors, parts, outs = [], [], [], []

        def score(g):
            query = jnp.concatenate([qs[h * G + g], onehot[...]], axis=1)
            sc = lax.dot_general(keys, query, CONTRACT_LAST, preferred_element_type=jnp.float32)
            head = jnp.minimum(sc[:ROWS], masks[phase])
            held[g, :ROWS] = head
            held[g, ROWS:width] = sc[ROWS:]
            new = jnp.maximum(olds[g], jnp.max(head, axis=0, keepdims=True))
            new = jnp.maximum(new, jnp.max(sc[ROWS:], axis=0, keepdims=True))
            news.append(new)
            factors.append(jnp.exp2((olds[g] - new) * EXP_SCALE))

        def soften(g):
            level = news[g] * EXP_SCALE
            part = jnp.zeros((8, ROWS), jnp.float32)
            for at in range(0, width, CHUNK):
                w = jnp.exp2(held[g, at:at + CHUNK] * EXP_SCALE - level)
                for row in range(0, CHUNK, 8):
                    part = part + w[row:row + 8]
                weights[g, at:at + CHUNK] = w.astype(jnp.bfloat16)
            parts.append(jnp.sum(part, axis=0, keepdims=True))

        def gather(g):
            outs.append(
                lax.dot_general(
                    vals, weights[g, :width], CONTRACT_FIRST, preferred_element_type=jnp.float32
                )
            )

        for g in range(AHEAD):
            score(g)
        for g in range(G):
            if g + AHEAD < G:
                score(g + AHEAD)
            soften(g)
            gather(g)
        for g in range(G):
            i = h * G + g
            best[i] = news[g]
            total[i] = sums[g] * factors[g] + parts[g]
            acc[i] = acc[i] * factors[g] + outs[g]

    rank = 2 * c + z

    def block_lists(k, r):
        near = [(0, 0, r // 2)] + [
            (0, flip, core) for core in range(2) for flip in range(2) if 2 * core + ((r % 2) ^ flip) < r
        ]
        same, cross = [(1, 0, 0), (1, 0, 1)], [(1, 1, 0), (1, 1, 1)]
        far = [(2, 0, core) for core in range(2) if 2 * core + r % 2 >= r]
        far_cross = [(2, 1, core) for core in range(2) if 2 * core + 1 - r % 2 >= r]
        if k == 0:
            first, second = near, []
        elif k == 2:
            spare = 2 - min(r, 2)
            first = near + cross[: 1 if r == 3 else 2] + far[:spare]
            second = (cross[1:] if r == 3 else []) + same + far[spare:] + far_cross
        else:
            first = near + same[: 1 if r == 3 else 2]
            second = (same[1:] if r == 3 else []) + cross + (far + far_cross if k == 3 else [])
        pad = [(k + 1, 0, 0)] * 3
        first = first + pad[: max(0, 3 - len(first))]
        second = second + (pad[: max(0, 3 - len(second))] if second else [])
        return first, second

    lists = {(k, r): block_lists(k, r) for k in range(4) for r in range(4)}

    def chosen_by_place(value):
        result = 0
        for (k, r), pair in lists.items():
            result = jnp.where((y == k) & (rank == r), value(pair), result)
        return result

    def resolve(phase, at):
        def field(n):
            return chosen_by_place(lambda pair: (pair[phase] + [(3, 0, 0)] * 6)[at][n])

        back, flip, core = field(0), field(1), field(2)
        place = slot(jnp.minimum(back, 3), core, z + flip - 2 * z * flip)
        masked = back > y
        at_bias = jnp.where(masked, 12, 4 * jnp.minimum(back, 2) + 2 * flip + core)
        return jnp.where(masked, own_slot, place), at_bias

    sizes = [chosen_by_place(lambda pair, phase=phase: len(pair[phase])) for phase in range(2)]
    resolved = [[resolve(phase, at) for at in range(6)] for phase in range(2)]

    def compute(phase, h):
        size = jnp.where(phase == 0, sizes[0], sizes[1])
        for count in range(3, 7):
            @pl.when(size == count)
            def _():
                update(
                    [jnp.where(phase == 0, resolved[0][at][0], resolved[1][at][0]) for at in range(count)],
                    [jnp.where(phase == 0, resolved[0][at][1], resolved[1][at][1]) for at in range(count)],
                    phase,
                    h,
                )

    sib = 1 - c

    def block(at_y, core, zz):
        return 4 * at_y + 2 * zz + core

    def on(condition, h, source, *onward):
        @pl.when(condition)
        def _():
            arrived(source, h)
            for link, ok, sem in onward:
                if ok is True:
                    send(link, source, h, sem)
                else:
                    @pl.when(ok)
                    def _(link=link, sem=sem):
                        send(link, source, h, sem)

    other = 1 - z
    home = [block(k, c, z) for k in range(4)]
    away = [block(k, c, other) for k in range(4)]
    sib_home = [block(k, sib, z) for k in range(4)]
    sib_away = [block(k, sib, other) for k in range(4)]
    to_sib = (SIBLING, True, None)

    def within(t, low, high):
        return (t >= low) & (t < high)

    def serve_0(t):
        on(t < 8, t, away[0], (UP, t < 6, None), to_sib)
        on(t < 8, t, home[1], (DOWN, True, None))

    def serve_1(t):
        on(t < 8, t, away[1], (UP, True, None), to_sib)
        on(t < 8, t, home[0], (UP, t >= 6, None), (ACROSS, t >= 6, None), to_sib)
        on(within(t, 8, 14), t - 8, away[0], to_sib)
        on(within(t, 10, 12), t - 4, away[0], (UP, True, None), to_sib)

    def serve_2(t):
        on(t < 8, t, away[2], (UP, t < 6, None), to_sib)
        on(t < 2, t, home[1], to_sib)
        on(within(t, 2, 8), t - 2, home[0], (ACROSS, True, None), to_sib)
        on(within(t, 2, 10), t - 2, away[1], to_sib)
        on(within(t, 10, 12), t - 4, home[0], to_sib)
        on(within(t, 9, 15), t - 9, away[0], to_sib)
        on(within(t, 10, 16), t - 8, home[1], to_sib)
        on(within(t, 12, 14), t - 6, away[0], to_sib)

    def serve_3(t):
        on(within(t, 1, 7), t - 1, home[0], (DOWN, True, None))
        on(
            within(t, 7, 15), t - 7, home[1],
            (DOWN, t >= 9, None), (ACROSS, gives_far, 5), to_sib,
        )
        on(t < 8, t, home[2], (ACROSS, t >= 6, None), to_sib)
        on((t < 8) & takes_own, t, away[3], (SIBLING, True, 6))
        on(within(t, 8, 14), t - 8, away[2], to_sib)
        on(within(t, 9, 11), t - 3, away[2], to_sib)
        on(within(t, 10, 18) & takes_far, t - 10, away[1], (SIBLING, True, 7))

    def early_0(h):
        arrived(sib_away[0], h)

    def early_1(h):
        arrived(sib_away[1], h)
        arrived(sib_home[0], h)

    def early_2(h):
        arrived(sib_away[2], h)
        arrived(sib_away[1], h)
        arrived(sib_home[0], h)

    def early_3(h):
        on(sib_takes_own, h, sib_away[3])
        arrived(sib_home[2], h)

    def late_0(h):
        pass

    def late_1(h):
        arrived(sib_away[0], h)

    def late_2(h):
        arrived(sib_home[1], h)
        arrived(sib_away[0], h)

    def late_3(h):
        arrived(sib_away[2], h)
        arrived(sib_home[1], h)
        on(sib_takes_far, h, sib_away[1])

    late_after = jnp.where(y == 3, LATE, LATE - 1)

    @pl.loop(0, 8 + LATE)
    def _(t):
        for k, serve in enumerate((serve_0, serve_1, serve_2, serve_3)):
            @pl.when(y == k)
            def _(serve=serve):
                serve(t)

        early_h = jnp.where(y == 2, jnp.where(t < 10, t - 3, t - 5), t - 1)
        late_h = t - late_after
        early = jnp.where(y == 2, within(t, 3, 9) | within(t, 11, 13), within(t, 1, 9))
        late = within(late_h, 0, 8)

        @pl.when(early)
        def _():
            arrived(slot(0, sib, z), early_h)
            for k, wait in enumerate((early_0, early_1, early_2, early_3)):
                @pl.when(y == k)
                def _(wait=wait):
                    wait(early_h)

        @pl.when(late)
        def _():
            for k, wait in enumerate((late_0, late_1, late_2, late_3)):
                @pl.when(y == k)
                def _(wait=wait):
                    wait(late_h)

        @pl.loop(0, 2)
        def _(phase):
            @pl.when(jnp.where(phase == 0, early, late))
            def _():
                compute(phase, jnp.where(phase == 0, early_h, late_h))

        @pl.when(late)
        def _():
            for g in range(G):
                i = late_h * G + g
                out_ref[:, pl.ds(pl.multiple_of(i * D, D), D)] = (
                    (acc[i] / total[i]).T.astype(jnp.bfloat16)
                )

    counts = ((14, 14, 8, 16), (14, 8, 10, 32), (14, 0, 14, 48), (0, 12, 2, 32))
    for k in range(4):
        @pl.when(y == k)
        def _(k=k):
            for link in range(4):
                sent(link, counts[k][link])

    @pl.when(y == 3)
    def _():
        for sem, used in ((4, gives_own), (5, gives_far), (6, takes_own), (7, takes_far)):
            @pl.when(used)
            def _(sem=sem):
                sent(sem, KH)


def local(queries, keys, values, positions, doc_lengths):
    any_space = pl.BlockSpec(memory_space=pl.ANY)
    vmem = pl.BlockSpec(memory_space=pltpu.VMEM)
    bf16, f32 = jnp.bfloat16, jnp.float32
    heads = KH * G
    return pl.pallas_call(
        kernel,
        out_shape=pltpu.VMEM(queries.shape, bf16),
        in_specs=[any_space, any_space, any_space, vmem, pl.BlockSpec(memory_space=pltpu.SMEM)],
        out_specs=vmem,
        scratch_shapes=[
            pltpu.VMEM((16 * KH, 2 * ROWS, D), bf16),
            pltpu.VMEM((ROWS, heads * D), bf16),
            pltpu.VMEM((heads, ROWS, D), bf16),
            pltpu.VMEM((ROWS, KH * D), bf16),
            pltpu.VMEM((heads, D, ROWS), f32),
            pltpu.VMEM((heads, 1, ROWS), f32),
            pltpu.VMEM((heads, 1, ROWS), f32),
            pltpu.VMEM((G, 6 * ROWS, ROWS), f32),
            pltpu.VMEM((G, 6 * ROWS, ROWS), bf16),
            pltpu.VMEM((2, ROWS, ROWS), f32),
            pltpu.VMEM((13, ROWS, D), bf16),
            pltpu.VMEM((ROWS, D), bf16),
            pltpu.VMEM((ROWS, D), f32),
            pltpu.VMEM((ROWS, D), f32),
            pltpu.SemaphoreType.DMA((2,)),
            pltpu.SemaphoreType.DMA((KH,)),
            pltpu.SemaphoreType.DMA((8,)),
            pltpu.SemaphoreType.DMA((128,)),
        ],
        compiler_params=pltpu.CompilerParams(
            collective_id=0, has_side_effects=True, vmem_limit_bytes=56 * 1024 * 1024
        ),
    )(queries, keys, values, positions, doc_lengths)


def solution(mesh):
    rows = ("seq", "blk", "uly")
    in_specs = (P(rows, None), P(rows, None), P(rows, None), P(None, rows), P("seq"))
    return jax.shard_map(
        local, mesh=mesh, in_specs=in_specs, out_specs=P(rows, None), check_vma=False
    )
```
